256 devices in a mesh: date: 16 (over z, core), book: 16 (over x, y).
Axes of the slice: x: 4, y: 4, z: 8, core: 2. Of those that a mesh axis runs over, the one named last changes fastest.
Arguments:
- shocks: bfloat16 [32, 512, 8192], P('date', None, 'book'), may hold values from -6 to 6
- persistence: float32 [8192], P('book'), may hold values from 0.5 to 1
- volatility: float32 [8192], P('book'), may hold values from 0.05 to 0.4
- base_rate: float32 [8192], P('book'), may hold values from 0 to 1
- cashflows: bfloat16 [65536, 512], P('book'), may hold values from -0.0625 to 0.0625
- block_owner: int32 [256, 1], P('book'), may hold values from 0 to 15; in each aligned block of 16 rows (0 to 15, 16 to 31, ...) at most 2 rows name the same one
- trade_set: int32 [65536], P('book'), may hold values from 0 to 511
- threshold: float32 [512], P('book'), may hold values from 0.1 to 1
- margin_lag: int32 [512], P('book'), may hold values from 1 to 2
Outputs:
- net_value: float32 [32, 512, 512], P('date', None, 'book')
- expected_exposure: float32 [32, 512], P('date', 'book')
The draws below stay inside these ranges and needn't reach their ends.
Inputs may be any that keep to these rules, and one draw needn't show every extreme that they name: `block_owner`: among the blocks of one index of book, no value is named by more than 2 blocks.
All inputs are finite; a program needn't handle non-finite values.
Results may differ from the reference program's by a relative error of at most 0.0039.
Values may be sent and summed in bfloat16 or wider, within the bound.
A program may use at most 128 MiB of HBM per device.

```python
import math
import jax
import jax.numpy as jnp
import numpy as np
from jax import lax

CF = 512
SETS = 512
TB = 256
DATE_DEV = 2
PATHS = 512
BLK_DEV = 16
MOST = 2
DATES = 32
BUCKETS = 8192
BLOCKS = 256
TRADES = 65536
N_BOOK = 16


def touch_ends(array, own_key, least, largest):
    shape = array.shape
    index_at = [jax.random.randint(jax.random.fold_in(own_key, axis), (), 0, shape[axis]) for axis in range(len(shape))]
    array = array.at[tuple(index_at)].set(least)
    longest = shape.index(max(shape))
    index_at[longest] = (index_at[longest] + 1) % shape[longest]
    return array.at[tuple(index_at)].set(largest)


def level_of(rng, shape, shards, least, top_value):
    factor_of = 1.0
    for dim, parts in shards:
        heights = jax.random.uniform(jax.random.fold_in(jax.random.fold_in(rng, 6), dim), (parts,), jnp.float32, least / len(shards), top_value / len(shards))
        factor_of = factor_of * jnp.repeat(jnp.exp(heights), shape[dim] // parts).reshape((-1,) + (1,) * (len(shape) - 1 - dim))
    return factor_of


def assign_block(rng, own, number, rows, number_of, top, limit, slope):
    order = jax.random.permutation(rng, number_of)
    crowded, common = shares(number_of, rows * top, limit, slope, True), shares(number_of, rows * top, limit, slope, False)
    places = jnp.arange(number_of)

    def named(lengths, turn):
        used = int((lengths > 0).sum())
        fixed = max(1, used // 4)
        passed = fixed + (places - fixed + turn * (used - fixed)) % max(1, number_of - fixed)
        return jnp.zeros((number_of,), jnp.int32).at[order[jnp.where(places < fixed, places, passed)]].set(jnp.asarray(lengths, jnp.int32))

    lengths = jnp.where(number % 4 == 0, named(crowded, number // 4), named(common, number - number // 4 - 1))
    mixed = jax.random.permutation(jax.random.fold_in(own, 3), number_of)
    giver, taker = mixed[0:number_of // 2 * 2:2], mixed[1:number_of // 2 * 2:2]
    margin = jnp.minimum(lengths[giver] - 1, limit - lengths[taker]) // 2
    margin = jnp.where((giver == order[0]) | (taker == order[0]) | (lengths[taker] == 0), 0, jnp.maximum(margin, 0))
    passed = jax.random.randint(jax.random.fold_in(own, 4), (number_of // 2,), 0, 1 << 20) % (margin + 1)
    lengths = lengths.at[giver].add(-passed).at[taker].add(passed)
    items = jnp.searchsorted(jnp.cumsum(lengths), jnp.arange(rows * top), side="right").astype(jnp.int32)
    listing = items.reshape(top, rows).T
    listing = listing[jax.random.permutation(jax.random.fold_in(own, 1), rows)]
    turn = jax.random.randint(jax.random.fold_in(own, 2), (rows, 1), 0, top)
    return jnp.take_along_axis(listing, (jnp.arange(top)[None, :] + turn) % top, axis=1)


def shares(count, total, most, slope, full):
    portions = [(1 << 20) // math.isqrt(standing ** slope) + 1 for standing in range(1, count + 1)]
    largest = most if full else min(most, max(-(-total // count), total * portions[0] // sum(portions)))
    least = 1 if total - largest >= count - 1 else 0
    counts, spare = [largest] + [least] * (count - 1), total - largest - least * (count - 1)
    while spare > 0:
        free = [i for i in range(1, count) if counts[i] < largest] or [i for i in range(1, count) if counts[i] < most]
        whole, budget = sum([portions[i] for i in free]), spare
        for i in free:
            extra = min(most - counts[i], max(1, budget * portions[i] // whole), spare)
            counts[i] = counts[i] + extra
            spare = spare - extra
    return np.array(counts)


def scatter_about(stream_key, dims, width, bound, shards=(), held_as=jnp.bfloat16):
    drawn = jax.random.normal(stream_key, dims, jnp.float32) * width
    if len(shards) > 0:
        drawn = level_of(stream_key, dims, shards, -0.22, 0.18) * drawn
    return jnp.clip(drawn, min=-bound, max=bound).astype(held_as)


def setup_inputs(seed: int = 0) -> dict:
    key_list = jax.random.split(jax.random.key(seed), 10)
    shocks = scatter_about(key_list[0], (DATES, PATHS, BUCKETS), 1.0, 6.0, ((0, 16), (2, 16)))
    persistence = jnp.clip(0.5 + 0.5 * jax.random.uniform(key_list[1], (BUCKETS,), jnp.float32) ** level_of(key_list[1], (BUCKETS,), ((0, 16),), -0.2, 0.2), 0.5, 1.0)
    volatility = jnp.clip(jnp.exp(math.log(0.4) - 2.0794415 * jax.random.uniform(key_list[2], (BUCKETS,), jnp.float32) ** level_of(key_list[2], (BUCKETS,), ((0, 16),), -0.2, 0.2)), 0.05, 0.4)
    base_rate = jnp.clip(1.0 * jax.random.uniform(key_list[3], (BUCKETS,), jnp.float32) ** level_of(key_list[3], (BUCKETS,), ((0, 16),), -0.2, 0.2), 0.0, 1.0)
    cashflows = scatter_about(key_list[4], (TRADES, CF), (2.0 * (CF * TRADES // SETS) ** -0.5), 0.0625, ((0, 16),))
    block_owner_keys = jax.random.split(jax.random.fold_in(key_list[5], 1), BLOCKS // BLK_DEV)
    block_owner_turns = jax.random.permutation(jax.random.fold_in(key_list[5], 3), BLOCKS // BLK_DEV)
    block_owner = jax.vmap(lambda own, number: assign_block(jax.random.fold_in(key_list[5], 2), own, number, BLK_DEV, N_BOOK, 1, MOST, 2))(block_owner_keys, block_owner_turns).reshape((BLOCKS, 1))
    trade_set = touch_ends(jax.random.randint(key_list[6], (TRADES,), 0, SETS), jax.random.fold_in(key_list[6], 1), 0, SETS - 1).astype(jnp.int32)
    threshold = jnp.clip(jnp.exp(math.log(1.0) - 2.3025851 * jax.random.uniform(key_list[7], (SETS,), jnp.float32) ** level_of(key_list[7], (SETS,), ((0, 16),), -0.2, 0.2)), 0.1, 1.0)
    margin_lag = touch_ends(jax.random.randint(key_list[8], (SETS,), 1, DATE_DEV + 1), jax.random.fold_in(key_list[8], 1), 1, DATE_DEV).astype(jnp.int32)
    return {"shocks": shocks, "persistence": persistence, "volatility": volatility, "base_rate": base_rate, "cashflows": cashflows, "block_owner": block_owner, "trade_set": trade_set, "threshold": threshold, "margin_lag": margin_lag}


def reference(shocks, persistence, volatility, base_rate, cashflows, block_owner, trade_set, threshold, margin_lag):
    def advance(state, shock):
        state = persistence * state + volatility * shock.astype(jnp.float32)
        return state, state

    start = jnp.zeros((PATHS, BUCKETS), jnp.float32)
    _, level = lax.scan(advance, start, shocks)
    discount = jnp.exp(-(base_rate + level)).astype(jnp.bfloat16)
    flat = discount.reshape(DATES * PATHS, BUCKETS)
    owners = block_owner[:, 0].astype(jnp.int32)
    cf_blocks = cashflows.reshape(BLOCKS, TB, CF)
    set_blocks = trade_set.reshape(BLOCKS, TB)
    labels = jnp.arange(SETS, dtype=jnp.int32)

    def add_block(total, item):
        owner, flows, sets = item
        slab = lax.dynamic_slice_in_dim(flat, (owner * CF).astype(jnp.int32), CF, 1)
        price = jnp.dot(slab, flows.T, preferred_element_type=jnp.float32).astype(jnp.bfloat16)
        onehot = (sets[:, None] == labels[None, :]).astype(jnp.bfloat16)
        return total + jnp.dot(price, onehot, preferred_element_type=jnp.float32), None

    total = jnp.zeros((DATES * PATHS, SETS), jnp.float32)
    total, _ = lax.scan(add_block, total, (owners, cf_blocks, set_blocks))
    net_value = total.reshape(DATES, PATHS, SETS)
    collateral = jnp.zeros_like(net_value)
    for lag in range(1, DATE_DEV + 1):
        moved = jnp.concatenate([jnp.zeros((lag, PATHS, SETS), jnp.float32), net_value[:DATES - lag]], 0)
        collateral = jnp.where(margin_lag[None, None, :] == lag, moved, collateral)
    exposure = jnp.maximum(net_value - collateral - threshold[None, None, :], 0.0)
    return net_value, jnp.mean(exposure, axis=1)
```

```python
import functools

import jax
import jax.numpy as jnp
from jax import lax
from jax.experimental import pallas as pl
from jax.experimental.pallas import tpu as pltpu
from jax.sharding import PartitionSpec as P

MESH = pl.DeviceIdType.MESH
LANES = 128
CHUNKS = 2
F32, BF16 = jnp.float32, jnp.bfloat16


def kernel(
    nd,
    nb,
    shocks,
    persistence,
    volatility,
    base_rate,
    cashflows,
    owner,
    trade_set,
    threshold,
    margin_lag,
    net_out,
    exposure_out,
    flows,
    tile_of,
    outgoing,
    incoming,
    weights,
    factors,
    discount,
    partial,
    arrived,
    packed,
    returned,
    local_sem,
    a_send,
    a_recv,
    b_send,
    b_recv,
    c_send,
    c_recv,
    h_send,
    h_recv,
    e_send,
    e_recv,
    f_send,
    f_recv,
):
    d, o = lax.axis_index("date"), lax.axis_index("book")
    nz = nd // 2
    z, core = d // 2, d % 2
    dates = shocks.shape[0]
    width = shocks.shape[2]
    total_dates = dates * nd
    here = shocks.shape[1] // nd
    piece = here // CHUNKS
    blocks = tile_of.shape[0] - 1
    block_rows = flows.shape[0] // blocks
    set_rows = tile_of.shape[1]
    own_sets = net_out.shape[1]
    column_tiles = width // LANES

    def column_of(index):
        return pl.multiple_of((index % column_tiles) * LANES, LANES)

    def row_of(index):
        return pl.multiple_of((index // column_tiles) * set_rows, set_rows)

    def tile(index):
        return weights.at[pl.ds(row_of(index), set_rows), pl.ds(column_of(index), LANES)]

    barrier = pltpu.get_barrier_semaphore()

    @pl.loop(1, nd)
    def _(i):
        pl.semaphore_signal(barrier, 1, device_id={"date": (d + i) % nd}, device_id_type=MESH)

    @pl.loop(1, nb)
    def _(i):
        pl.semaphore_signal(barrier, 1, device_id={"book": (o + i) % nb}, device_id_type=MESH)

    load = pltpu.make_async_copy(
        cashflows.at[:, pl.ds(column_of(d), LANES)], flows, local_sem.at[CHUNKS]
    )
    load.start()

    def paths_of(q, k):
        return pl.ds(pl.multiple_of(q * here + k * piece, piece), piece)

    def own_factors(k):
        return pltpu.make_async_copy(
            shocks.at[:, paths_of(d, k), :],
            factors.at[k, pl.ds(d * dates, dates)],
            local_sem.at[k],
        )

    for k in range(CHUNKS):
        own_factors(k).start()

    load.wait()
    first_set = (d // column_tiles) * set_rows
    labels = lax.broadcasted_iota(jnp.int32, (set_rows, LANES), 0) + first_set
    rows_each = block_rows // LANES
    for b in range(blocks):
        hot = jnp.concatenate(
            [
                jnp.where(labels == trade_set[b * rows_each + r : b * rows_each + r + 1, :], 1.0, 0.0)
                for r in range(rows_each)
            ],
            axis=1,
        ).astype(BF16)
        tile_of[b] = jnp.dot(
            hot, flows[b * block_rows : (b + 1) * block_rows, :], preferred_element_type=F32
        )
    tile_of[blocks] = jnp.zeros((set_rows, LANES), F32)

    @pl.loop(0, nb)
    def _(target):
        first, second = jnp.int32(blocks), jnp.int32(blocks)
        for b in reversed(range(blocks)):
            named = owner[0, b] == target
            second = jnp.where(named, first, second)
            first = jnp.where(named, b, first)
        outgoing[target] = (tile_of[first] + tile_of[second]).astype(BF16)

    pl.semaphore_wait(barrier, nd + nb - 2)

    def send_factors(i, k):
        q = (d + i) % nd
        return pltpu.make_async_remote_copy(
            src_ref=shocks.at[:, paths_of(q, k), :],
            dst_ref=factors.at[k, pl.ds(d * dates, dates)],
            send_sem=a_send.at[k, q],
            recv_sem=a_recv.at[k, d],
            device_id={"date": q},
            device_id_type=MESH,
        )

    def got_factors(i, k):
        q = (d + i) % nd
        return pltpu.make_async_remote_copy(
            src_ref=shocks.at[:, paths_of(q, k), :],
            dst_ref=factors.at[k, pl.ds(q * dates, dates)],
            send_sem=a_send.at[k, q],
            recv_sem=a_recv.at[k, q],
            device_id={"date": q},
            device_id_type=MESH,
        )

    def send_tile(i):
        q = (o + i) % nb
        return pltpu.make_async_remote_copy(
            src_ref=outgoing.at[q],
            dst_ref=incoming.at[o],
            send_sem=b_send.at[q],
            recv_sem=b_recv.at[o],
            device_id={"book": q},
            device_id_type=MESH,
        )

    def got_tile(i):
        q = (o + i) % nb
        return pltpu.make_async_remote_copy(
            src_ref=outgoing.at[q],
            dst_ref=incoming.at[q],
            send_sem=b_send.at[q],
            recv_sem=b_recv.at[q],
            device_id={"book": q},
            device_id_type=MESH,
        )

    pl.loop(1, nb)(lambda i: send_tile(i).start())
    pl.loop(1, nd)(lambda i: send_factors(i, 0).start())
    pl.loop(1, nb)(lambda i: got_tile(i).wait_recv())

    summed = lax.fori_loop(
        1,
        nb,
        lambda i, total: total + incoming[(o + i) % nb].astype(F32),
        outgoing[o].astype(F32),
    )
    weights[pl.ds(row_of(d), set_rows), pl.ds(column_of(d), LANES)] = summed.astype(BF16)

    def spread(i, sender):
        q = (z + i) % nz
        mine = tile(sender)
        return pltpu.make_async_remote_copy(
            src_ref=mine,
            dst_ref=mine,
            send_sem=c_send.at[q],
            recv_sem=c_recv.at[sender // 2],
            device_id={"date": q * 2 + core},
            device_id_type=MESH,
        )

    def handed(index, from_core):
        at = tile(index * 2 + from_core)
        return pltpu.make_async_remote_copy(
            src_ref=at,
            dst_ref=at,
            send_sem=h_send.at[index],
            recv_sem=h_recv.at[index],
            device_id={"date": d + 1 - 2 * core},
            device_id_type=MESH,
        )

    pl.loop(1, nz)(lambda i: spread(i, d).start())
    handed(z, core).start()
    for k in range(1, CHUNKS):
        pl.loop(1, nd)(lambda i: send_factors(i, k).start())

    keep = persistence[...]
    scale = volatility[...]
    base = base_rate[...]

    def discounts(k):
        own_factors(k).wait()
        pl.loop(1, nd)(lambda i: got_factors(i, k).wait_recv())

        def step(t, level):
            level = keep * level + scale * factors[k, t].astype(F32)
            rows = pl.ds(pl.multiple_of(t * piece, piece), piece)
            discount[rows, :] = jnp.exp(-(base + level)).astype(BF16)
            return level

        lax.fori_loop(0, total_dates, step, jnp.zeros((piece, width), F32), unroll=4)

    def send_partial(i, k):
        q = (o + i) % nb
        return pltpu.make_async_remote_copy(
            src_ref=partial.at[k, pl.ds(pl.multiple_of(q * own_sets, own_sets), own_sets), :],
            dst_ref=arrived.at[k, o],
            send_sem=e_send.at[k, q],
            recv_sem=e_recv.at[k, o],
            device_id={"book": q},
            device_id_type=MESH,
        )

    def got_partial(i, k):
        q = (o + i) % nb
        return pltpu.make_async_remote_copy(
            src_ref=partial.at[k, pl.ds(pl.multiple_of(q * own_sets, own_sets), own_sets), :],
            dst_ref=arrived.at[k, q],
            send_sem=e_send.at[k, q],
            recv_sem=e_recv.at[k, q],
            device_id={"book": q},
            device_id_type=MESH,
        )

    def values(k):
        partial[k] = lax.dot_general(
            weights[...], discount[...], (((1,), (1,)), ((), ())), preferred_element_type=F32
        ).astype(BF16)
        pl.loop(1, nb)(lambda i: send_partial(i, k).start())

    discounts(0)

    @pl.loop(1, nz)
    def _(i):
        q = (z + i) % nz
        spread(i, q * 2 + core).wait_recv()
        handed(q, core).start()

    pl.loop(0, nz)(lambda i: handed(i, 1 - core).wait_recv())
    values(0)
    for k in range(1, CHUNKS):
        discounts(k)
        values(k)

    lane = lax.broadcasted_iota(jnp.int32, (8, LANES), 1)
    groups = LANES // own_sets
    bands = own_sets // 8
    lane_block = lane // own_sets
    lane_piece = lane // piece

    def swapped(tiles):
        out = []
        for m in range(groups):
            made = None
            for a in range(groups):
                shift = ((a - m) * own_sets) % LANES
                moved = pltpu.roll(tiles[a], shift, 1) if shift else tiles[a]
                made = moved if made is None else jnp.where(lane_block == a, moved, made)
            out.append(made)
        return out

    def send_back(i, k):
        q = (d + i) % nd
        depth = 16 if k == CHUNKS - 1 else 8
        return pltpu.make_async_remote_copy(
            src_ref=packed.at[k, q, pl.ds(0, depth), :],
            dst_ref=returned.at[k, d, pl.ds(0, depth), :],
            send_sem=f_send.at[k, q],
            recv_sem=f_recv.at[k, d],
            device_id={"date": q},
            device_id_type=MESH,
        )

    def got_back(i, k):
        q = (d + i) % nd
        depth = 16 if k == CHUNKS - 1 else 8
        return pltpu.make_async_remote_copy(
            src_ref=packed.at[k, q, pl.ds(0, depth), :],
            dst_ref=returned.at[k, q, pl.ds(0, depth), :],
            send_sem=f_send.at[k, q],
            recv_sem=f_recv.at[k, q],
            device_id={"date": q},
            device_id_type=MESH,
        )

    lags = margin_lag[...].reshape(1, 1, own_sets)
    limits = threshold[...].reshape(1, 1, own_sets)
    packed[CHUNKS - 1, :, 8:16, :] = jnp.zeros((nd, 8, LANES), F32)
    exposure = jnp.zeros((total_dates, own_sets), F32)
    for k in range(CHUNKS):
        pl.loop(1, nb)(lambda i: got_partial(i, k).wait_recv())
        own = partial[k, pl.ds(pl.multiple_of(o * own_sets, own_sets), own_sets), :]
        net = lax.fori_loop(
            1,
            nb,
            lambda i, total: total + arrived[k, (o + i) % nb].astype(F32),
            own.astype(F32),
        )
        for g in range(total_dates * piece // LANES):
            tiles = [net[a * 8 : a * 8 + 8, g * LANES : (g + 1) * LANES] for a in range(bands)]
            for m, made in enumerate(swapped(tiles)):
                packed[k, g * groups + m, 0:8, :] = made
        if k < CHUNKS - 1:
            pl.loop(1, nd)(lambda i: send_back(i, k).start())
        by_date = net.T.reshape(total_dates, piece, own_sets)
        zero = jnp.zeros((1, piece, own_sets), F32)
        once = jnp.concatenate([zero, by_date[:-1]], axis=0)
        twice = jnp.concatenate([zero, once[:-1]], axis=0)
        collateral = jnp.where(lags == 1, once, jnp.where(lags == 2, twice, 0.0))
        exposure += jnp.sum(jnp.maximum(by_date - collateral - limits, 0.0), axis=1)
    for q in range(nd):
        packed[CHUNKS - 1, q, 8 : 8 + dates, 0:own_sets] = exposure[q * dates : (q + 1) * dates, :]
    pl.loop(1, nd)(lambda i: send_back(i, CHUNKS - 1).start())

    mean = jnp.zeros((dates, own_sets), F32)
    for k in range(CHUNKS):
        depth = 16 if k == CHUNKS - 1 else 8
        returned[k, d, 0:depth, :] = packed[k, d, 0:depth, :]
        pl.loop(1, nd)(lambda i: got_back(i, k).wait_recv())
        for g in range(nd // groups):
            lanes = slice(g * LANES, (g + 1) * LANES)
            tiles = [returned[k, g * groups + m, 0:8, :] for m in range(groups)]
            for a in range(bands):
                for t in range(dates):
                    rows = slice(a * 8, a * 8 + 8)
                    made = None if k == 0 else net_out[t, rows, lanes]
                    for m in range(groups):
                        shift = (m * here + k * piece - a * own_sets - t * piece) % LANES
                        moved = pltpu.roll(tiles[m], shift, 1) if shift else tiles[m]
                        chosen = lane_piece == m * CHUNKS + k
                        made = moved if made is None else jnp.where(chosen, moved, made)
                    net_out[t, rows, lanes] = made
    for q in range(nd):
        mean += returned[CHUNKS - 1, q, 8 : 8 + dates, 0:own_sets]
    exposure_out[...] = mean * (1.0 / shocks.shape[1])

    for k in range(CHUNKS):
        pl.loop(1, nd)(lambda i: send_factors(i, k).wait_send())
        pl.loop(1, nb)(lambda i: send_partial(i, k).wait_send())
        pl.loop(1, nd)(lambda i: send_back(i, k).wait_send())
    pl.loop(1, nb)(lambda i: send_tile(i).wait_send())
    pl.loop(1, nz)(lambda i: spread(i, d).wait_send())
    pl.loop(0, nz)(lambda i: handed(i, core).wait_send())


def on_device(
    nd,
    nb,
    shocks,
    persistence,
    volatility,
    base_rate,
    cashflows,
    block_owner,
    trade_set,
    threshold,
    margin_lag,
):
    dates, paths, width = shocks.shape
    trades = cashflows.shape[0]
    blocks = block_owner.shape[0]
    own_sets = threshold.shape[0]
    sets = own_sets * nb
    set_rows = sets * width // (nd * LANES)
    here = paths // nd
    piece = here // CHUNKS
    rows = dates * nd * piece
    nz = nd // 2
    vmem = pl.BlockSpec(memory_space=pltpu.VMEM)
    anywhere = pl.BlockSpec(memory_space=pl.ANY)
    dma = pltpu.SemaphoreType.DMA
    net_value, exposure = pl.pallas_call(
        functools.partial(kernel, nd, nb),
        out_shape=(
            jax.ShapeDtypeStruct((dates, own_sets, paths), F32),
            jax.ShapeDtypeStruct((dates, own_sets), F32),
        ),
        in_specs=[
            anywhere,
            vmem,
            vmem,
            vmem,
            anywhere,
            pl.BlockSpec(memory_space=pltpu.SMEM),
            vmem,
            vmem,
            vmem,
        ],
        out_specs=(vmem, vmem),
        scratch_shapes=[
            pltpu.VMEM((trades, LANES), BF16),
            pltpu.VMEM((blocks + 1, set_rows, LANES), F32),
            pltpu.VMEM((nb, set_rows, LANES), BF16),
            pltpu.VMEM((nb, set_rows, LANES), BF16),
            pltpu.VMEM((sets, width), BF16),
            pltpu.VMEM((CHUNKS, dates * nd, piece, width), BF16),
            pltpu.VMEM((rows, width), BF16),
            pltpu.VMEM((CHUNKS, sets, rows), BF16),
            pltpu.VMEM((CHUNKS, nb, own_sets, rows), BF16),
            pltpu.VMEM((CHUNKS, nd, 16, LANES), F32),
            pltpu.VMEM((CHUNKS, nd, 16, LANES), F32),
            dma((CHUNKS + 1,)),
            dma((CHUNKS, nd)),
            dma((CHUNKS, nd)),
            dma((nb,)),
            dma((nb,)),
            dma((nz,)),
            dma((nz,)),
            dma((nz,)),
            dma((nz,)),
            dma((CHUNKS, nb)),
            dma((CHUNKS, nb)),
            dma((CHUNKS, nd)),
            dma((CHUNKS, nd)),
        ],
        compiler_params=pltpu.CompilerParams(collective_id=0, has_side_effects=True),
    )(
        shocks,
        persistence.reshape(1, width),
        volatility.reshape(1, width),
        base_rate.reshape(1, width),
        cashflows,
        block_owner.reshape(1, blocks),
        trade_set.reshape(trades // LANES, LANES),
        threshold.reshape(1, own_sets),
        margin_lag.reshape(1, own_sets),
    )
    return net_value.swapaxes(1, 2), exposure


def solution(mesh):
    return jax.shard_map(
        functools.partial(on_device, mesh.shape["date"], mesh.shape["book"]),
        mesh=mesh,
        in_specs=(
            P("date", None, "book"),
            P("book"),
            P("book"),
            P("book"),
            P("book", None),
            P("book", None),
            P("book"),
            P("book"),
            P("book"),
        ),
        out_specs=(P("date", None, "book"), P("date", "book")),
        check_vma=False,
    )
```

```python
import functools

import jax
import jax.numpy as jnp
from jax import lax
from jax.experimental import pallas as pl
from jax.experimental.pallas import tpu as pltpu
from jax.sharding import PartitionSpec as P

MESH = pl.DeviceIdType.MESH
LANES = 128
CHUNKS = 2
PARTS = 2
STEPS = 32700.0
LARGEST = 6.0
F32, BF16 = jnp.float32, jnp.bfloat16


def kernel(
    nd,
    nb,
    shocks,
    persistence,
    volatility,
    base_rate,
    cashflows,
    owner,
    trade_set,
    threshold,
    margin_lag,
    net_out,
    exposure_out,
    flows,
    tile_of,
    outgoing,
    incoming,
    weights,
    lent,
    factors,
    carried,
    gathered,
    prefixes,
    state,
    discount,
    partial,
    arrived,
    net,
    earlier,
    sums,
    sums_got,
    local_sem,
    s_send,
    s_recv,
    a_send,
    a_recv,
    p_send,
    p_recv,
    b_send,
    b_recv,
    c_send,
    c_recv,
    h_send,
    h_recv,
    e_send,
    e_recv,
    l_send,
    l_recv,
    n_send,
    n_recv,
    m_send,
    m_recv,
):
    d, o = lax.axis_index("date"), lax.axis_index("book")
    nz = nd // 2
    z, core = d // 2, d % 2
    other = 1 - core
    dates = shocks.shape[0]
    width = shocks.shape[2]
    span = 2 * dates
    half = shocks.shape[1] // 2
    some = half // CHUNKS
    piece = some // nz
    blocks = tile_of.shape[0] - 1
    block_rows = flows.shape[0] // blocks
    set_rows = tile_of.shape[1]
    part_rows = set_rows // PARTS
    own_sets = net_out.shape[1]
    column_tiles = width // LANES
    partner = {"date": d + 1 - 2 * core}

    def send(src, dst, out_sem, in_sem, where):
        return pltpu.make_async_remote_copy(
            src_ref=src,
            dst_ref=dst,
            send_sem=out_sem,
            recv_sem=in_sem,
            device_id=where,
            device_id_type=MESH,
        )

    def tile(index, h):
        rows = pl.multiple_of((index // column_tiles) * part_rows, part_rows)
        columns = pl.multiple_of((index % column_tiles) * LANES, LANES)
        return h, pl.ds(rows, part_rows), pl.ds(columns, LANES)

    barrier = pltpu.get_barrier_semaphore()

    @pl.loop(1, nd)
    def _(i):
        pl.semaphore_signal(barrier, 1, device_id={"date": (d + i) % nd}, device_id_type=MESH)

    @pl.loop(1, nb)
    def _(i):
        pl.semaphore_signal(barrier, 1, device_id={"book": (o + i) % nb}, device_id_type=MESH)

    columns = pl.ds(pl.multiple_of((d % column_tiles) * LANES, LANES), LANES)
    load = pltpu.make_async_copy(cashflows.at[:, columns], flows, local_sem.at[0])
    load.start()

    def paths_of(c, k):
        return pl.ds(pl.multiple_of(c * half + k * some, some), some)

    mine = pl.ds(core * dates, dates)
    theirs = pl.ds(other * dates, dates)

    def lend(k):
        return pltpu.make_async_copy(
            shocks.at[:, paths_of(other, k), :], lent.at[k], local_sem.at[1 + k]
        )

    def retain(k):
        return pltpu.make_async_copy(
            shocks.at[:, paths_of(core, k), :],
            factors.at[k, mine],
            local_sem.at[1 + CHUNKS + k],
        )

    for k in range(CHUNKS):
        lend(k).start()
        retain(k).start()

    load.wait()
    first_set = (d // column_tiles) * set_rows
    labels = lax.broadcasted_iota(jnp.int32, (set_rows, LANES), 0) + first_set
    rows_each = block_rows // LANES
    for b in range(blocks):
        hot = jnp.concatenate(
            [
                jnp.where(labels == trade_set[b * rows_each + r : b * rows_each + r + 1, :], 1.0, 0.0)
                for r in range(rows_each)
            ],
            axis=1,
        ).astype(BF16)
        tile_of[b] = jnp.dot(
            hot, flows[b * block_rows : (b + 1) * block_rows, :], preferred_element_type=F32
        )
    tile_of[blocks] = jnp.zeros((set_rows, LANES), F32)

    @pl.loop(0, nb)
    def _(target):
        first, second = jnp.int32(blocks), jnp.int32(blocks)
        for b in reversed(range(blocks)):
            named = owner[0, b] == target
            second = jnp.where(named, first, second)
            first = jnp.where(named, b, first)
        outgoing[target] = (tile_of[first] + tile_of[second]).astype(BF16)

    keep = persistence[...]
    scale = volatility[...]
    base = base_rate[...]
    keep_span = keep
    bound_one = 1.0 + keep
    for _ in range(span - 2):
        bound_one = 1.0 + keep * bound_one
    for _ in range(span - 1):
        keep_span = keep_span * keep
    bound_one = bound_one * scale * LARGEST
    to_steps = STEPS / bound_one
    from_steps = bound_one * (1.0 / STEPS)

    for k in range(CHUNKS):
        lend(k).wait()
        retain(k).wait()

    pl.semaphore_wait(barrier, nd + nb - 2)

    def swap_shocks(k, slot):
        return send(lent.at[k], factors.at[k, slot], s_send.at[k], s_recv.at[k], partner)

    def send_tile(i, h):
        q = (o + i) % nb
        rows = pl.ds(h * part_rows, part_rows)
        return send(
            outgoing.at[q, rows], incoming.at[o, rows], b_send.at[h, q], b_recv.at[h, o], {"book": q}
        )

    def got_tile(i, h):
        q = (o + i) % nb
        rows = pl.ds(h * part_rows, part_rows)
        return send(
            outgoing.at[q, rows], incoming.at[q, rows], b_send.at[h, q], b_recv.at[h, q], {"book": q}
        )

    for k in range(CHUNKS):
        swap_shocks(k, mine).start()
    for h in range(PARTS):
        pl.loop(1, nb)(lambda i: send_tile(i, h).start())

    def send_carry(i, k):
        q = (z + i) % nz
        return send(
            carried.at[k, q],
            gathered.at[k, z],
            a_send.at[k, q],
            a_recv.at[k, z],
            {"date": q * 2 + core},
        )

    def got_carry(i, k):
        q = (z + i) % nz
        return send(
            carried.at[k, q],
            gathered.at[k, q],
            a_send.at[k, q],
            a_recv.at[k, q],
            {"date": q * 2 + core},
        )

    for k in range(CHUNKS):
        swap_shocks(k, theirs).wait_recv()

        @pl.loop(0, nz)
        def _(q):
            rows = pl.ds(pl.multiple_of(q * piece, piece), piece)
            total = scale * factors[k, 0, rows, :].astype(F32)
            for t in range(1, span):
                total = keep * total + scale * factors[k, t, rows, :].astype(F32)
            carried[k, q] = jnp.round(total * to_steps).astype(jnp.int32).astype(jnp.int16)

        gathered[k, z] = carried[k, z]
        pl.loop(1, nz)(lambda i: send_carry(i, k).start())

    def spread(i, sender, h):
        q = (z + i) % nz
        at = tile(sender, h)
        return send(
            weights.at[at],
            weights.at[at],
            c_send.at[h, q],
            c_recv.at[h, sender // 2],
            {"date": q * 2 + core},
        )

    def handed(index, from_core, h):
        at = tile(index * 2 + from_core, h)
        return send(weights.at[at], weights.at[at], h_send.at[h, index], h_recv.at[h, index], partner)

    def sum_tiles(h):
        pl.loop(1, nb)(lambda i: got_tile(i, h).wait_recv())
        rows = pl.ds(h * part_rows, part_rows)
        summed = lax.fori_loop(
            1,
            nb,
            lambda i, total: total + incoming[(o + i) % nb, rows, :].astype(F32),
            outgoing[o, rows, :].astype(F32),
        )
        weights[tile(d, h)] = summed.astype(BF16)
        pl.loop(1, nz)(lambda i: spread(i, d, h).start())
        handed(z, core, h).start()

    def send_prefix(i, k):
        q = (z + i) % nz
        return send(
            prefixes.at[k, q], state.at[k, z], p_send.at[k, q], p_recv.at[k, z], {"date": q * 2 + core}
        )

    def got_prefix(i, k):
        q = (z + i) % nz
        return send(
            prefixes.at[k, q], state.at[k, q], p_send.at[k, q], p_recv.at[k, q], {"date": q * 2 + core}
        )

    def prefix(k):
        pl.loop(1, nz)(lambda i: got_carry(i, k).wait_recv())
        level = jnp.zeros((piece, width), F32)
        bound = jnp.zeros_like(bound_one)
        for q in range(nz):
            if q == 0:
                prefixes[k, q] = jnp.zeros((piece, width), jnp.int16)
            else:
                prefixes[k, q] = (
                    jnp.round(level * (STEPS / bound)).astype(jnp.int32).astype(jnp.int16)
                )
            level = keep_span * level + gathered[k, q].astype(F32) * from_steps
            bound = keep_span * bound + bound_one
        state[k, z] = prefixes[k, z]
        pl.loop(1, nz)(lambda i: send_prefix(i, k).start())

    for k in range(max(CHUNKS, PARTS)):
        if k < PARTS:
            sum_tiles(k)
        if k < CHUNKS:
            prefix(k)

    bound_here = jnp.zeros_like(bound_one)
    for q in range(nz - 1):
        bound_here = jnp.where(q < z, keep_span * bound_here + bound_one, bound_here)
    unit = bound_here * (1.0 / STEPS)

    def discounts(k):
        pl.loop(1, nz)(lambda i: got_prefix(i, k).wait_recv())

        @pl.loop(0, nz)
        def _(q):
            rows = pl.ds(pl.multiple_of(q * piece, piece), piece)
            level = state[k, q].astype(F32) * unit
            for t in range(span):
                level = keep * level + scale * factors[k, t, rows, :].astype(F32)
                at = pl.ds(pl.multiple_of(t * some + q * piece, piece), piece)
                discount[k, at, :] = jnp.exp(-(base + level)).astype(BF16)

    def partial_at(q):
        first = q * own_sets
        inside = first % set_rows
        start = (first // set_rows) * part_rows + inside % part_rows
        return inside // part_rows, pl.ds(pl.multiple_of(start, own_sets), own_sets)

    def book_at(h, i):
        each = part_rows // own_sets
        return (i // each) * (set_rows // own_sets) + h * each + i % each

    def send_partial(q, k):
        h, rows = partial_at(q)
        return send(
            partial.at[k, h, rows, :], arrived.at[k, o], e_send.at[k, q], e_recv.at[k, o], {"book": q}
        )

    def got_partial(i, k):
        q = (o + i) % nb
        h, rows = partial_at(q)
        return send(
            partial.at[k, h, rows, :], arrived.at[k, q], e_send.at[k, q], e_recv.at[k, q], {"book": q}
        )

    def values(k, h):
        partial[k, h] = lax.dot_general(
            weights[h], discount[k], (((1,), (1,)), ((), ())), preferred_element_type=F32
        ).astype(BF16)

        @pl.loop(0, nb // PARTS)
        def _(i):
            q = book_at(h, i)

            @pl.when(q != o)
            def _():
                send_partial(q, k).start()

    def forward(h):
        @pl.loop(1, nz)
        def _(i):
            q = (z + i) % nz
            spread(i, q * 2 + core, h).wait_recv()
            handed(q, core, h).start()

    forward(0)
    discounts(0)
    for h in range(PARTS):
        if h:
            forward(h)
        pl.loop(0, nz)(lambda i: handed(i, other, h).wait_recv())
        values(0, h)
    for k in range(1, CHUNKS):
        discounts(k)
        for h in range(PARTS):
            values(k, h)

    def send_earlier(k):
        return send(
            net.at[k, :, pl.ds((span - 2) * some, 2 * some)],
            earlier.at[k],
            l_send.at[k],
            l_recv.at[k],
            {"date": (d + 2) % nd},
        )

    def send_net(k, t, c):
        lanes = pl.ds(pl.multiple_of(((1 - c) * dates + t) * some, some), some)
        return send(
            net.at[k, :, lanes],
            net_out.at[t, :, paths_of(c, k)],
            n_send.at[k, t],
            n_recv.at[k, t],
            partner,
        )

    for k in range(CHUNKS):
        pl.loop(1, nb)(lambda i: got_partial(i, k).wait_recv())
        at, rows = partial_at(o)
        net[k] = lax.fori_loop(
            1,
            nb,
            lambda i, total: total + arrived[k, (o + i) % nb].astype(F32),
            partial[k, at, rows, :].astype(F32),
        )

        @pl.when(z < nz - 1)
        def _():
            send_earlier(k).start()

        for t in range(dates):
            send_net(k, t, core).start()

    lags = jnp.broadcast_to(margin_lag[...], (8, own_sets)).T[:, 0:1]
    limits = jnp.broadcast_to(threshold[...], (8, own_sets)).T[:, 0:1]
    sums[...] = jnp.zeros_like(sums)
    totals = [jnp.zeros((own_sets, some), F32) for _ in range(span)]
    for k in range(CHUNKS):
        for t in range(dates):
            lanes = pl.ds(pl.multiple_of((core * dates + t) * some, some), some)
            net_out[t, :, paths_of(core, k)] = net[k, :, lanes]

        @pl.when(z > 0)
        def _():
            send_earlier(k).wait_recv()

        @pl.when(z == 0)
        def _():
            earlier[k] = jnp.zeros((own_sets, 2 * some), F32)

        known = [earlier[k, :, 0:some], earlier[k, :, some : 2 * some]]
        known += [net[k, :, t * some : (t + 1) * some] for t in range(span)]
        for t in range(span):
            collateral = jnp.where(lags == 1, known[t + 1], jnp.where(lags == 2, known[t], 0.0))
            totals[t] += jnp.maximum(known[t + 2] - collateral - limits, 0.0)
    for t in range(span):
        row = jnp.sum(totals[t].T, axis=0, keepdims=True)
        sums[t // dates, t % dates : t % dates + 1, 0:own_sets] = row

    swap_sums = send(sums.at[other], sums_got, m_send, m_recv, partner)
    swap_sums.start()
    for k in range(CHUNKS):
        for t in range(dates):
            send_net(k, t, other).wait_recv()
    swap_sums.wait_recv()
    both = sums[core, 0:dates, 0:own_sets] + sums_got[0:dates, 0:own_sets]
    exposure_out[...] = both * (1.0 / shocks.shape[1])

    swap_sums.wait_send()
    for k in range(CHUNKS):
        swap_shocks(k, mine).wait_send()
        pl.loop(1, nz)(lambda i: send_carry(i, k).wait_send())
        pl.loop(1, nz)(lambda i: send_prefix(i, k).wait_send())
        pl.loop(1, nb)(lambda i: send_partial((o + i) % nb, k).wait_send())

        @pl.when(z < nz - 1)
        def _():
            send_earlier(k).wait_send()

        for t in range(dates):
            send_net(k, t, core).wait_send()
    for h in range(PARTS):
        pl.loop(1, nb)(lambda i: send_tile(i, h).wait_send())
        pl.loop(1, nz)(lambda i: spread(i, d, h).wait_send())
        pl.loop(0, nz)(lambda i: handed(i, core, h).wait_send())


def on_device(
    nd,
    nb,
    shocks,
    persistence,
    volatility,
    base_rate,
    cashflows,
    block_owner,
    trade_set,
    threshold,
    margin_lag,
):
    dates, paths, width = shocks.shape
    trades = cashflows.shape[0]
    blocks = block_owner.shape[0]
    own_sets = threshold.shape[0]
    sets = own_sets * nb
    set_rows = sets * width // (nd * LANES)
    nz = nd // 2
    some = paths // 2 // CHUNKS
    piece = some // nz
    rows = 2 * dates * some
    vmem = pl.BlockSpec(memory_space=pltpu.VMEM)
    anywhere = pl.BlockSpec(memory_space=pl.ANY)
    dma = pltpu.SemaphoreType.DMA
    net_value, exposure = pl.pallas_call(
        functools.partial(kernel, nd, nb),
        out_shape=(
            jax.ShapeDtypeStruct((dates, own_sets, paths), F32),
            jax.ShapeDtypeStruct((dates, own_sets), F32),
        ),
        in_specs=[
            anywhere,
            vmem,
            vmem,
            vmem,
            anywhere,
            pl.BlockSpec(memory_space=pltpu.SMEM),
            vmem,
            vmem,
            vmem,
        ],
        out_specs=(vmem, vmem),
        scratch_shapes=[
            pltpu.VMEM((trades, LANES), BF16),
            pltpu.VMEM((blocks + 1, set_rows, LANES), F32),
            pltpu.VMEM((nb, set_rows, LANES), BF16),
            pltpu.VMEM((nb, set_rows, LANES), BF16),
            pltpu.VMEM((PARTS, sets // PARTS, width), BF16),
            pltpu.VMEM((CHUNKS, dates, some, width), BF16),
            pltpu.VMEM((CHUNKS, 2 * dates, some, width), BF16),
            pltpu.VMEM((CHUNKS, nz, piece, width), jnp.int16),
            pltpu.VMEM((CHUNKS, nz, piece, width), jnp.int16),
            pltpu.VMEM((CHUNKS, nz, piece, width), jnp.int16),
            pltpu.VMEM((CHUNKS, nz, piece, width), jnp.int16),
            pltpu.VMEM((CHUNKS, rows, width), BF16),
            pltpu.VMEM((CHUNKS, PARTS, sets // PARTS, rows), BF16),
            pltpu.VMEM((CHUNKS, nb, own_sets, rows), BF16),
            pltpu.VMEM((CHUNKS, own_sets, rows), F32),
            pltpu.VMEM((CHUNKS, own_sets, 2 * some), F32),
            pltpu.VMEM((2, 8, LANES), F32),
            pltpu.VMEM((8, LANES), F32),
            dma((1 + 2 * CHUNKS,)),
            dma((CHUNKS,)),
            dma((CHUNKS,)),
            dma((CHUNKS, nz)),
            dma((CHUNKS, nz)),
            dma((CHUNKS, nz)),
            dma((CHUNKS, nz)),
            dma((PARTS, nb)),
            dma((PARTS, nb)),
            dma((PARTS, nz)),
            dma((PARTS, nz)),
            dma((PARTS, nz)),
            dma((PARTS, nz)),
            dma((CHUNKS, nb)),
            dma((CHUNKS, nb)),
            dma((CHUNKS,)),
            dma((CHUNKS,)),
            dma((CHUNKS, dates)),
            dma((CHUNKS, dates)),
            dma,
            dma,
        ],
        compiler_params=pltpu.CompilerParams(collective_id=0, has_side_effects=True),
    )(
        shocks,
        persistence.reshape(1, width),
        volatility.reshape(1, width),
        base_rate.reshape(1, width),
        cashflows,
        block_owner.reshape(1, blocks),
        trade_set.reshape(trades // LANES, LANES),
        threshold.reshape(1, own_sets),
        margin_lag.reshape(1, own_sets),
    )
    return net_value.swapaxes(1, 2), exposure


def solution(mesh):
    return jax.shard_map(
        functools.partial(on_device, mesh.shape["date"], mesh.shape["book"]),
        mesh=mesh,
        in_specs=(
            P("date", None, "book"),
            P("book"),
            P("book"),
            P("book"),
            P("book", None),
            P("book", None),
            P("book"),
            P("book"),
            P("book"),
        ),
        out_specs=(P("date", None, "book"), P("date", "book")),
        check_vma=False,
    )
```

```python
import functools

import jax
import jax.numpy as jnp
from jax import lax
from jax.experimental import pallas as pl
from jax.experimental.pallas import tpu as pltpu
from jax.sharding import PartitionSpec as P

MESH = pl.DeviceIdType.MESH
LANES = 128
CHUNKS = 2
PARTS = 2
SPREADING = (("tiles", 0), ("states", 0), ("tiles", 1), ("states", 1))
PRICING = (
    ("forward", 0),
    ("discounts", 0),
    ("handed", 0),
    ("values", 0, 0),
    ("forward", 1),
    ("handed", 1),
    ("values", 0, 1),
    ("discounts", 1),
    ("values", 1, 0),
    ("values", 1, 1),
)
STEPS = 32700.0
LARGEST = 6.0
F32, BF16 = jnp.float32, jnp.bfloat16


def kernel(
    nd,
    nb,
    shocks,
    keep_hbm,
    scale_hbm,
    base_hbm,
    cashflows,
    owner_hbm,
    sets_hbm,
    limits_hbm,
    lags_hbm,
    net_out,
    exposure_out,
    keep_ref,
    scale_ref,
    base_ref,
    owner,
    trade_set,
    limits_ref,
    lags_ref,
    flows,
    tile_of,
    outgoing,
    incoming,
    weights,
    lent,
    factors,
    carried,
    gathered,
    prefixes,
    state,
    discount,
    partial,
    arrived,
    net,
    other_net,
    earlier,
    local_sem,
    s_send,
    s_recv,
    a_send,
    a_recv,
    p_send,
    p_recv,
    b_send,
    b_recv,
    c_send,
    c_recv,
    h_send,
    h_recv,
    e_send,
    e_recv,
    l_send,
    l_recv,
    n_send,
    n_recv,
):
    d, o = lax.axis_index("date"), lax.axis_index("book")
    nz = nd // 2
    z, core = d // 2, d % 2
    other = 1 - core
    dates = shocks.shape[0]
    width = shocks.shape[2]
    span = 2 * dates
    half = shocks.shape[1] // 2
    some = half // CHUNKS
    piece = some // nz
    blocks = tile_of.shape[0] - 1
    block_rows = flows.shape[0] // blocks
    set_rows = tile_of.shape[1]
    part_rows = set_rows // PARTS
    own_sets = net_out.shape[1]
    column_tiles = width // LANES
    partner = {"date": d + 1 - 2 * core}

    def send(src, dst, out_sem, in_sem, where):
        return pltpu.make_async_remote_copy(
            src_ref=src,
            dst_ref=dst,
            send_sem=out_sem,
            recv_sem=in_sem,
            device_id=where,
            device_id_type=MESH,
        )

    def tile(index, h):
        rows = pl.multiple_of((index // column_tiles) * part_rows, part_rows)
        columns = pl.multiple_of((index % column_tiles) * LANES, LANES)
        return h, pl.ds(rows, part_rows), pl.ds(columns, LANES)

    columns = pl.ds(pl.multiple_of((d % column_tiles) * LANES, LANES), LANES)
    loads = [
        pltpu.make_async_copy(src, dst, local_sem.at[2 * CHUNKS + n])
        for n, (src, dst) in enumerate(
            [
                (cashflows.at[:, columns], flows),
                (sets_hbm, trade_set),
                (owner_hbm, owner),
                (keep_hbm, keep_ref),
                (scale_hbm, scale_ref),
                (base_hbm, base_ref),
                (limits_hbm, limits_ref),
                (lags_hbm, lags_ref),
            ]
        )
    ]
    for load in loads:
        load.start()

    barrier = pltpu.get_barrier_semaphore()

    @pl.loop(1, nd)
    def _(i):
        pl.semaphore_signal(barrier, 1, device_id={"date": (d + i) % nd}, device_id_type=MESH)

    @pl.loop(1, nb)
    def _(i):
        pl.semaphore_signal(barrier, 1, device_id={"book": (o + i) % nb}, device_id_type=MESH)

    def paths_of(c, k):
        return pl.ds(pl.multiple_of(c * half + k * some, some), some)

    mine = pl.ds(core * dates, dates)
    theirs = pl.ds(other * dates, dates)

    def lend(k):
        return pltpu.make_async_copy(
            shocks.at[:, paths_of(other, k), :], lent.at[k], local_sem.at[k]
        )

    def retain(k):
        return pltpu.make_async_copy(
            shocks.at[:, paths_of(core, k), :],
            factors.at[k, mine],
            local_sem.at[CHUNKS + k],
        )

    for k in range(CHUNKS):
        lend(k).start()
        retain(k).start()

    for load in loads:
        load.wait()
    first_set = (d // column_tiles) * set_rows
    row = lax.broadcasted_iota(jnp.int32, (set_rows, LANES), 0)
    spaced = (row % part_rows) // own_sets * PARTS + row // part_rows
    labels = first_set + spaced * own_sets + row % own_sets
    rows_each = block_rows // LANES
    for b in range(blocks):
        hot = jnp.concatenate(
            [
                jnp.where(labels == trade_set[b * rows_each + r : b * rows_each + r + 1, :], 1.0, 0.0)
                for r in range(rows_each)
            ],
            axis=1,
        ).astype(BF16)
        tile_of[b] = jnp.dot(
            hot, flows[b * block_rows : (b + 1) * block_rows, :], preferred_element_type=F32
        )
    tile_of[blocks] = jnp.zeros((set_rows, LANES), F32)

    @pl.loop(0, nb)
    def _(target):
        first, second = jnp.int32(blocks), jnp.int32(blocks)
        for b in reversed(range(blocks)):
            named = owner[0, b] == target
            second = jnp.where(named, first, second)
            first = jnp.where(named, b, first)
        made = (tile_of[first] + tile_of[second]).astype(BF16)
        for h in range(PARTS):
            outgoing[h, target] = made[h * part_rows : (h + 1) * part_rows, :]

    keep = keep_ref[...]
    scale = scale_ref[...]
    base = base_ref[...]
    keep_span = keep
    bound_one = 1.0 + keep
    for _ in range(span - 2):
        bound_one = 1.0 + keep * bound_one
    for _ in range(span - 1):
        keep_span = keep_span * keep
    bound_one = bound_one * scale * LARGEST
    to_steps = STEPS / bound_one
    from_steps = bound_one * (1.0 / STEPS)

    for k in range(CHUNKS):
        lend(k).wait()
        retain(k).wait()

    pl.semaphore_wait(barrier, nd + nb - 2)

    def swap_shocks(k, slot):
        return send(lent.at[k], factors.at[k, slot], s_send, s_recv.at[k], partner)

    def send_tile(i, h):
        q = (o + i) % nb
        return send(outgoing.at[h, q], incoming.at[h, o], b_send.at[h], b_recv.at[h], {"book": q})

    def all_of(src, dst, out_sem, in_sem):
        return send(src, dst, out_sem, in_sem, partner)

    for k in range(CHUNKS):
        swap_shocks(k, mine).start()
    for h in range(PARTS):
        pl.loop(1, nb)(lambda i: send_tile(i, h).start())

    def send_carry(i, k):
        q = (z + i) % nz
        return send(
            carried.at[k, q], gathered.at[k, z], a_send.at[k], a_recv.at[k], {"date": q * 2 + core}
        )

    for k in range(CHUNKS):
        swap_shocks(k, theirs).wait_recv()

        @pl.loop(0, nz)
        def _(q):
            rows = pl.ds(pl.multiple_of(q * piece, piece), piece)
            total = scale * factors[k, 0, rows, :].astype(F32)
            for t in range(1, span):
                total = keep * total + scale * factors[k, t, rows, :].astype(F32)
            carried[k, q] = jnp.round(total * to_steps).astype(jnp.int32).astype(jnp.int16)

        gathered[k, z] = carried[k, z]
        pl.loop(1, nz)(lambda i: send_carry(i, k).start())

    def spread(i, h):
        at = tile(d, h)
        return send(
            weights.at[at],
            weights.at[at],
            c_send.at[h],
            c_recv.at[h],
            {"date": ((z + i) % nz) * 2 + core},
        )

    def handed(index, h):
        at = tile(index * 2 + core, h)
        return send(weights.at[at], weights.at[at], h_send.at[h], h_recv.at[h], partner)

    tile_rows = part_rows * LANES // width

    def tiles(count, h, out_sem, in_sem):
        some_rows = weights.at[h, pl.ds(0, count * tile_rows)]
        return all_of(some_rows, some_rows, out_sem.at[h], in_sem.at[h])

    def got_tiles(h):
        some_tiles = incoming.at[h, pl.ds(0, nb - 1)]
        return all_of(some_tiles, some_tiles, b_send.at[h], b_recv.at[h])

    def sum_tiles(h):
        got_tiles(h).wait_recv()
        summed = lax.fori_loop(
            1,
            nb,
            lambda i, total: total + incoming[h, (o + i) % nb].astype(F32),
            outgoing[h, o].astype(F32),
        )
        weights[tile(d, h)] = summed.astype(BF16)
        pl.loop(1, nz)(lambda i: spread(i, h).start())
        handed(z, h).start()

    def send_prefix(i, k):
        q = (z + i) % nz
        return send(
            prefixes.at[k, q], state.at[k, z], p_send.at[k], p_recv.at[k], {"date": q * 2 + core}
        )

    def slices(src, dst, k, out_sem, in_sem):
        count = pl.ds(0, nz - 1)
        return all_of(src.at[k, count], dst.at[k, count], out_sem.at[k], in_sem.at[k])

    def prefix(k):
        slices(carried, gathered, k, a_send, a_recv).wait_recv()
        level = jnp.zeros((piece, width), F32)
        bound = jnp.zeros_like(bound_one)
        for q in range(nz):
            if q == 0:
                prefixes[k, q] = jnp.zeros((piece, width), jnp.int16)
            else:
                prefixes[k, q] = (
                    jnp.round(level * (STEPS / bound)).astype(jnp.int32).astype(jnp.int16)
                )
            level = keep_span * level + gathered[k, q].astype(F32) * from_steps
            bound = keep_span * bound + bound_one
        state[k, z] = prefixes[k, z]
        pl.loop(1, nz)(lambda i: send_prefix(i, k).start())

    for stage, index in SPREADING:
        (sum_tiles if stage == "tiles" else prefix)(index)

    bound_here = jnp.zeros_like(bound_one)
    for q in range(nz - 1):
        bound_here = jnp.where(q < z, keep_span * bound_here + bound_one, bound_here)
    unit = bound_here * (1.0 / STEPS)

    def discounts(k):
        slices(prefixes, state, k, p_send, p_recv).wait_recv()

        @pl.loop(0, nz)
        def _(q):
            rows = pl.ds(pl.multiple_of(q * piece, piece), piece)
            level = state[k, q].astype(F32) * unit
            for t in range(span):
                level = keep * level + scale * factors[k, t, rows, :].astype(F32)
                at = pl.ds(pl.multiple_of(t * some + q * piece, piece), piece)
                discount[k, at, :] = jnp.exp(-(base + level)).astype(BF16)

    holders = set_rows // own_sets
    each = part_rows // own_sets

    def partial_at(q):
        start = (q // holders) * part_rows + (q % holders) // PARTS * own_sets
        return q % PARTS, pl.ds(pl.multiple_of(start, own_sets), own_sets)

    def book_at(h, i):
        group = (o // holders + i // each) % (nb // holders)
        return group * holders + (o % holders + i) % each * PARTS + h

    def send_partial(q, k):
        h, rows = partial_at(q)
        return send(
            partial.at[k, h, rows, :], arrived.at[k, o], e_send.at[k], e_recv.at[k], {"book": q}
        )

    def partials(k):
        blocks_got = arrived.at[k, pl.ds(0, nb - 1)]
        return all_of(blocks_got, blocks_got, e_send.at[k], e_recv.at[k])

    def values(k, h):
        partial[k, h] = lax.dot_general(
            weights[h], discount[k], (((1,), (1,)), ((), ())), preferred_element_type=F32
        ).astype(BF16)

        @pl.loop(0, nb // PARTS)
        def _(i):
            q = book_at(h, i)

            @pl.when(q != o)
            def _():
                send_partial(q, k).start()

    def forward(h):
        tiles(nz - 1, h, c_send, c_recv).wait_recv()
        pl.loop(1, nz)(lambda i: handed((z + i) % nz, h).start())

    for stage, *index in PRICING:
        if stage == "forward":
            forward(*index)
        elif stage == "handed":
            tiles(nz, index[0], h_send, h_recv).wait_recv()
        elif stage == "discounts":
            discounts(*index)
        else:
            values(*index)

    def send_earlier(k):
        return send(
            net.at[k, :, pl.ds((span - 2) * some, 2 * some)],
            earlier.at[k, core],
            l_send.at[k],
            l_recv.at[k],
            {"date": ((z + 1) % nz) * 2},
        )

    def got_earlier(k):
        return all_of(earlier.at[k], earlier.at[k], l_send.at[k], l_recv.at[k])

    def swap_net(k):
        return send(net.at[k], other_net.at[k], n_send.at[k], n_recv.at[k], partner)

    def receive(k):
        partials(k).wait_recv()
        at, rows = partial_at(o)
        net[k] = lax.fori_loop(
            1,
            nb,
            lambda i, total: total + arrived[k, (o + i) % nb].astype(F32),
            partial[k, at, rows, :].astype(F32),
        )

        @pl.when(z < nz - 1)
        def _():
            send_earlier(k).start()

        swap_net(k).start()

    lags = jnp.broadcast_to(lags_ref[...], (8, own_sets)).T[:, 0:1]
    limits = jnp.broadcast_to(limits_ref[...], (8, own_sets)).T[:, 0:1]
    totals = [jnp.zeros((own_sets, some), F32) for _ in range(dates)]
    now = pl.ds(pl.multiple_of(core * dates * some, dates * some), dates * some)

    def settle(k):
        swap_net(k).wait_recv()

        @pl.when(core == 1)
        def _():
            earlier[k, core] = net[k, :, 0 : 2 * some]
            earlier[k, other] = other_net[k, :, 0 : 2 * some]

        @pl.when((core == 0) & (z == 0))
        def _():
            earlier[k] = jnp.zeros((2, own_sets, 2 * some), F32)

        for ref, side in ((net, core), (other_net, other)):
            values_now = ref[k, :, now]
            for t in range(dates):
                net_out[t, :, paths_of(side, k)] = values_now[:, t * some : (t + 1) * some]

        @pl.when((core == 0) & (z > 0))
        def _():
            got_earlier(k).wait_recv()

        for ref, side in ((net, core), (other_net, other)):
            past, values_now = earlier[k, side], ref[k, :, now]
            known = [past[:, 0:some], past[:, some : 2 * some]]
            known += [values_now[:, t * some : (t + 1) * some] for t in range(dates)]
            for t in range(dates):
                collateral = jnp.where(lags == 1, known[t + 1], jnp.where(lags == 2, known[t], 0.0))
                totals[t] += jnp.maximum(known[t + 2] - collateral - limits, 0.0)

    for k in range(CHUNKS):
        receive(k)
        if k:
            settle(k - 1)
    settle(CHUNKS - 1)
    for t in range(dates):
        row = jnp.sum(totals[t].T, axis=0, keepdims=True)
        exposure_out[t : t + 1, :] = row * (1.0 / shocks.shape[1])

    def finish_sends():
        for k in range(CHUNKS):
            slices(carried, gathered, k, a_send, a_recv).wait_send()
            slices(prefixes, state, k, p_send, p_recv).wait_send()
            partials(k).wait_send()

            @pl.when(z < nz - 1)
            def _():
                send_earlier(k).wait_send()

            swap_net(k).wait_send()
        all_of(lent, lent, s_send, s_recv.at[0]).wait_send()
        for h in range(PARTS):
            tiles(nz - 1, h, c_send, c_recv).wait_send()
            tiles(nz, h, h_send, h_recv).wait_send()
        for h in range(PARTS):
            got_tiles(h).wait_send()

    finish_sends()


def plain(net_ref, exposure_ref, net_out, exposure_out, sems):
    copies = [
        pltpu.make_async_copy(net_ref, net_out, sems.at[0]),
        pltpu.make_async_copy(exposure_ref, exposure_out, sems.at[1]),
    ]
    for copy in copies:
        copy.start()
    for copy in copies:
        copy.wait()


def on_device(
    nd,
    nb,
    shocks,
    persistence,
    volatility,
    base_rate,
    cashflows,
    block_owner,
    trade_set,
    threshold,
    margin_lag,
):
    dates, paths, width = shocks.shape
    trades = cashflows.shape[0]
    blocks = block_owner.shape[0]
    own_sets = threshold.shape[0]
    sets = own_sets * nb
    set_rows = sets * width // (nd * LANES)
    nz = nd // 2
    some = paths // 2 // CHUNKS
    piece = some // nz
    rows = 2 * dates * some
    vmem = pl.BlockSpec(memory_space=pltpu.VMEM)
    anywhere = pl.BlockSpec(memory_space=pl.ANY)
    dma = pltpu.SemaphoreType.DMA
    sent = pl.pallas_call(
        functools.partial(kernel, nd, nb),
        out_shape=(
            pltpu.VMEM((dates, own_sets, paths), F32),
            pltpu.VMEM((dates, own_sets), F32),
        ),
        in_specs=[anywhere] * 9,
        out_specs=(vmem, vmem),
        scratch_shapes=[
            pltpu.VMEM((1, width), F32),
            pltpu.VMEM((1, width), F32),
            pltpu.VMEM((1, width), F32),
            pltpu.SMEM((1, blocks), jnp.int32),
            pltpu.VMEM((trades // LANES, LANES), jnp.int32),
            pltpu.VMEM((1, own_sets), F32),
            pltpu.VMEM((1, own_sets), jnp.int32),
            pltpu.VMEM((trades, LANES), BF16),
            pltpu.VMEM((blocks + 1, set_rows, LANES), F32),
            pltpu.VMEM((PARTS, nb, set_rows // PARTS, LANES), BF16),
            pltpu.VMEM((PARTS, nb, set_rows // PARTS, LANES), BF16),
            pltpu.VMEM((PARTS, sets // PARTS, width), BF16),
            pltpu.VMEM((CHUNKS, dates, some, width), BF16),
            pltpu.VMEM((CHUNKS, 2 * dates, some, width), BF16),
            pltpu.VMEM((CHUNKS, nz, piece, width), jnp.int16),
            pltpu.VMEM((CHUNKS, nz, piece, width), jnp.int16),
            pltpu.VMEM((CHUNKS, nz, piece, width), jnp.int16),
            pltpu.VMEM((CHUNKS, nz, piece, width), jnp.int16),
            pltpu.VMEM((CHUNKS, rows, width), BF16),
            pltpu.VMEM((CHUNKS, PARTS, sets // PARTS, rows), BF16),
            pltpu.VMEM((CHUNKS, nb, own_sets, rows), BF16),
            pltpu.VMEM((CHUNKS, own_sets, rows), F32),
            pltpu.VMEM((CHUNKS, own_sets, rows), F32),
            pltpu.VMEM((CHUNKS, 2, own_sets, 2 * some), F32),
            dma((2 * CHUNKS + 8,)),
            dma,
            dma((CHUNKS,)),
            dma((CHUNKS,)),
            dma((CHUNKS,)),
            dma((CHUNKS,)),
            dma((CHUNKS,)),
            dma((PARTS,)),
            dma((PARTS,)),
            dma((PARTS,)),
            dma((PARTS,)),
            dma((PARTS,)),
            dma((PARTS,)),
            dma((CHUNKS,)),
            dma((CHUNKS,)),
            dma((CHUNKS,)),
            dma((CHUNKS,)),
            dma((CHUNKS,)),
            dma((CHUNKS,)),
        ],
        compiler_params=pltpu.CompilerParams(collective_id=0, has_side_effects=True),
    )(
        shocks,
        persistence.reshape(1, width),
        volatility.reshape(1, width),
        base_rate.reshape(1, width),
        cashflows,
        block_owner.reshape(1, blocks),
        trade_set.reshape(trades // LANES, LANES),
        threshold.reshape(1, own_sets),
        margin_lag.reshape(1, own_sets),
    )
    net_value, exposure = pl.pallas_call(
        plain,
        out_shape=tuple(jax.ShapeDtypeStruct(part.shape, F32) for part in sent),
        in_specs=[vmem, vmem],
        out_specs=(anywhere, anywhere),
        scratch_shapes=[dma((2,))],
    )(*(pltpu.with_memory_space_constraint(part, pltpu.VMEM) for part in sent))
    return net_value.swapaxes(1, 2), exposure


def solution(mesh):
    return jax.shard_map(
        functools.partial(on_device, mesh.shape["date"], mesh.shape["book"]),
        mesh=mesh,
        in_specs=(
            P("date", None, "book"),
            P("book"),
            P("book"),
            P("book"),
            P("book", None),
            P("book", None),
            P("book"),
            P("book"),
            P("book"),
        ),
        out_specs=(P("date", None, "book"), P("date", "book")),
        check_vma=False,
    )
```
